32 devices in a mesh: dp: 4 (over y, x), tensor: 8 (over z, core).
Axes of the slice: x: 2, y: 2, z: 4, core: 2. Of those that a mesh axis runs over, the one named last changes fastest.
Arguments:
- tokens: bfloat16 [2048, 4096], P(('dp', 'tensor')), parts along dimension 0, may hold values from -6 to 6
- norm_gain: float32 [4096], replicated, may hold values from 0.5 to 1.5
- gate_weight: bfloat16 [4096, 14336], P(None, 'tensor'), may hold values from -0.09375 to 0.09375
- up_weight: bfloat16 [4096, 14336], P(None, 'tensor'), may hold values from -0.09375 to 0.09375
- down_weight: bfloat16 [14336, 4096], P('tensor'), may hold values from -0.0625 to 0.0625
Outputs:
- mixed: bfloat16 [2048, 4096], P('dp', 'tensor'), parts along dimension 0
The draws below stay inside these ranges and needn't reach their ends.
There are 4 independent parts, one for each index of `dp`. The reference program is written for one: setup_inputs(seed, part) draws one part's arguments, and reference() takes and returns one part's arrays. A program takes and returns all parts, laid end to end along the dimension named above; an argument that names none is the same for every part. Nothing has to cross between parts.
All inputs are finite; a program needn't handle non-finite values.
Results may differ from the reference program's by a relative error of at most 0.0053.
Values may be sent and summed in bfloat16 or wider, within the bound.
A program may use at most 128 MiB of HBM per device.

```python
import jax
import jax.numpy as jnp
from jax import lax

D = 4096
FF = 14336
TOKENS = 512


def raised(entries, key, source, target, blocks, factor):
    owner, partner = [(jnp.arange(entries.shape[axis_at]) // (entries.shape[axis_at] // blocks)).reshape([-1 if axis == axis_at else 1 for axis in range(entries.ndim)]) for axis_at in (source, target)]
    chosen = jax.random.permutation(key, blocks)[partner]
    strong = (owner == chosen) | (owner == (partner + blocks // 2) % blocks)
    return jnp.where(strong, factor * entries, entries)


def levels(rng, extent, cuts, smallest, high):
    factor_of = 1.0
    for axis_at, parts in cuts:
        heights = jax.random.uniform(jax.random.fold_in(jax.random.fold_in(rng, 6), axis_at), (parts,), jnp.float32, smallest / len(cuts), high / len(cuts))
        factor_of = factor_of * jnp.repeat(jnp.exp(heights), extent[axis_at] // parts).reshape((-1,) + (1,) * (len(extent) - 1 - axis_at))
    return factor_of


def centred(stream_key, dims, spread, most, cuts=(), dtype=jnp.bfloat16):
    gain = levels(stream_key, dims, cuts, -0.22, 0.18) if cuts else 1.0
    drawn = jax.random.normal(stream_key, dims, jnp.float32) * spread * gain
    return jnp.minimum(jnp.maximum(drawn, -most), most).astype(dtype)


def bell_draw_with(rng, extent, spread, bound, shards, heavy, held_as=jnp.bfloat16):
    entries = spread * jax.random.normal(rng, extent, jnp.float32)
    if shards:
        entries = entries * levels(rng, extent, shards, -0.22, 0.18)
    return jnp.clip(raised(entries, jax.random.fold_in(rng, 3), *heavy), -bound, bound).astype(held_as)


def setup_inputs(seed: int = 0, part: int = 0) -> dict:
    streams_of = jax.random.split(jax.random.key(seed), 6)
    part_keys = jax.random.split(jax.random.fold_in(streams_of[5], part), 6)
    tokens = centred(part_keys[0], (TOKENS, D), 1.0, 6.0, ((0, 8),))
    norm_gain = jnp.clip(1.0 + 0.1 * jax.random.normal(streams_of[1], (D,), jnp.float32), 0.5, 1.5)
    gate_weight = centred(streams_of[2], (D, FF), D ** -0.5, 0.09375, ((1, 8),))
    up_weight = centred(streams_of[3], (D, FF), D ** -0.5, 0.09375, ((1, 8),))
    down_weight = bell_draw_with(streams_of[4], (FF, D), FF ** -0.5, 0.0625, ((0, 8),), (0, 1, 8, 2.0))
    return {"tokens": tokens, "norm_gain": norm_gain, "gate_weight": gate_weight, "up_weight": up_weight, "down_weight": down_weight}


def reference(tokens, norm_gain, gate_weight, up_weight, down_weight):
    wide = tokens.astype(jnp.float32)
    square_mean = lax.optimization_barrier(jnp.mean(wide * wide, axis=1, keepdims=True))
    normed = (wide * norm_gain[None, :] / jnp.sqrt(square_mean + 1e-05)).astype(jnp.bfloat16)
    gate = jnp.dot(normed, gate_weight, preferred_element_type=jnp.float32)
    up = jnp.dot(normed, up_weight, preferred_element_type=jnp.float32)
    hidden = (jax.nn.silu(gate) * up).astype(jnp.bfloat16)
    branch = jnp.dot(hidden, down_weight, preferred_element_type=jnp.float32)
    return (wide + branch).astype(jnp.bfloat16)
```

```python
import jax
import jax.numpy as jnp
from jax import lax
from jax.sharding import PartitionSpec as P


def on_device(tokens, norm_gain, gate_weight, up_weight, down_weight):
    n = lax.axis_size("tensor")
    me = lax.axis_index("tensor")
    every = lax.all_gather(tokens, "tensor", axis=0, tiled=True)
    wide = every.astype(jnp.float32)
    square_mean = jnp.mean(wide * wide, axis=1, keepdims=True)
    piece = (wide * norm_gain[None, :] / jnp.sqrt(square_mean + 1e-05)).astype(jnp.bfloat16)
    gate = jnp.dot(piece, gate_weight, preferred_element_type=jnp.float32)
    up = jnp.dot(piece, up_weight, preferred_element_type=jnp.float32)
    hidden = (jax.nn.silu(gate) * up).astype(jnp.bfloat16)
    width = every.shape[1] // n
    residual = lax.dynamic_slice_in_dim(every, me * width, width, axis=1)
    summed = lax.psum_scatter(
        jnp.einsum("fc,tf->ct", down_weight, hidden, preferred_element_type=jnp.float32).astype(jnp.bfloat16),
        "tensor",
        scatter_dimension=0,
        tiled=True,
    )
    return (residual.astype(jnp.float32) + summed.T.astype(jnp.float32)).astype(jnp.bfloat16)


def solution(mesh):
    return jax.shard_map(
        on_device,
        mesh=mesh,
        in_specs=(
            P(("dp", "tensor"), None),
            P(),
            P(None, "tensor"),
            P(None, "tensor"),
            P("tensor", None),
        ),
        out_specs=P("dp", "tensor"),
        check_vma=False,
    )
```

```python
import functools

import jax
import jax.numpy as jnp
from jax import lax
from jax.experimental import pallas as pl
from jax.experimental.pallas import tpu as pltpu
from jax.sharding import PartitionSpec as P

HALVES = 2
VMEM_LIMIT = 67043328


def block_kernel(
    n, tok, gain, gw, uw, dw, out,
    gwv, uwv, dwv, every, normed, hidden, part, peer, arrived, acc,
    load_sem, own_sem, ag_recv, ag_send, peer_send, peer_recv, rs_send, rs_recv,
):
    H = HALVES
    dp = lax.axis_index("dp")
    me = lax.axis_index("tensor")
    C = n // 2
    p, c = me // 2, me % 2
    rows, D = tok.shape
    r = rows // H
    T = n * r
    F = gwv.shape[1]
    width = D // n
    partner = (dp, 2 * p + (1 - c))
    right = (dp, lax.rem(me + 2, n))
    left = (dp, lax.rem(me + n - 2, n))
    has_right, has_left = p < C - 1, p > 0

    loads = [pltpu.make_async_copy(a, b, load_sem.at[k]) for k, (a, b) in enumerate(((gw, gwv), (uw, uwv), (dw, dwv)))]

    def block(h, t):
        return every.at[h, pl.ds(pl.multiple_of(t * r, r), r), :]

    own = [pltpu.make_async_copy(tok.at[pl.ds(h * r, r), :], block(h, me), own_sem.at[h]) for h in range(H)]
    for copy in own:
        copy.start()
    for copy in loads:
        copy.start()

    barrier = pltpu.get_barrier_semaphore()

    def greet(device):
        pl.semaphore_signal(barrier, inc=1, device_id=device, device_id_type=pl.DeviceIdType.MESH)

    greet(partner)
    pl.when(has_right)(lambda: greet(right))
    pl.when(has_left)(lambda: greet(left))
    pl.semaphore_wait(barrier, 1 + has_right.astype(jnp.int32) + has_left.astype(jnp.int32))

    def remote(src, dst, s, d, device):
        return pltpu.make_async_remote_copy(
            src_ref=src, dst_ref=dst, send_sem=s, recv_sem=d, device_id=device, device_id_type=pl.DeviceIdType.MESH
        )

    def gather(h, t, way):
        return remote(block(h, t), block(h, t), ag_send.at[way, h, t], ag_recv.at[h, t], (right, left, partner)[way])

    def gather_first(h):
        own[h].wait()
        pl.when(has_right)(lambda: gather(h, me, 0).start())
        pl.when(has_left)(lambda: gather(h, me, 1).start())
        gather(h, me, 2).start()

    def gather_step(h, s):
        @pl.when(p - s >= 0)
        def _():
            t = me - 2 * s
            gather(h, t, 2).wait_recv()
            pl.when(has_right)(lambda: gather(h, t, 0).start())
            gather(h, t, 2).start()

        @pl.when(p + s <= C - 1)
        def _():
            t = me + 2 * s
            gather(h, t, 2).wait_recv()
            pl.when(has_left)(lambda: gather(h, t, 1).start())
            gather(h, t, 2).start()

    def gather_last(h):
        for q in range(C):
            gather(h, 2 * q + (1 - c), 2).wait_recv()

    def gather_drain(h):
        for q in range(C):
            t = 2 * q + c
            pl.when((q <= p) & has_right)(lambda: gather(h, t, 0).wait_send())
            pl.when((q >= p) & has_left)(lambda: gather(h, t, 1).wait_send())
            gather(h, t, 2).wait_send()

    def to_peer(h, q):
        return remote(part.at[h, 2 * q + (1 - c)], peer.at[h, q], peer_send.at[h, q], peer_recv.at[h, q], partner)

    def to_right(h, q):
        return remote(part.at[h, 2 * q + c], arrived.at[h, q], rs_send.at[h, q], rs_recv.at[h, q], right)

    def to_left(h, q):
        slot = jnp.where(q == p - 1, C, q)
        return remote(part.at[h, 2 * q + c], arrived.at[h, slot], rs_send.at[h, q], rs_recv.at[h, slot], left)

    def landed(h, slot):
        remote(arrived.at[h, slot], arrived.at[h, slot], rs_send.at[h, 0], rs_recv.at[h, slot], partner).wait_recv()

    def scatter_first(h):
        for q in range(C):
            to_peer(h, q).wait_recv()
            t = 2 * q + c
            part[h, t] = (part[h, t].astype(jnp.float32) + peer[h, q].astype(jnp.float32)).astype(jnp.bfloat16)

        @pl.when(p == 0)
        def _():
            for q in reversed(range(1, C)):
                to_right(h, q).start()

        @pl.when(p == C - 1)
        def _():
            for q in range(C - 1):
                to_left(h, q).start()

    def add_arrived(h, q):
        landed(h, q)
        t = 2 * q + c
        part[h, t] = (part[h, t].astype(jnp.float32) + arrived[h, q].astype(jnp.float32)).astype(jnp.bfloat16)

    def scatter_step(h, j):
        def rightward():
            q = C - 1 - j

            @pl.when((q > p) & has_left)
            def _():
                add_arrived(h, q)
                to_right(h, q).start()

        def leftward():
            @pl.when((j < p) & has_right)
            def _():
                add_arrived(h, j)
                to_left(h, j).start()

        @pl.when(2 * p < C)
        def _():
            rightward()
            leftward()

        @pl.when(2 * p >= C)
        def _():
            leftward()
            rightward()

    def scatter_last(h):
        lanes = pl.ds(pl.multiple_of(me * width, width), width)
        acc[...] = every[h, :, lanes].astype(jnp.float32) + part[h, me].astype(jnp.float32)

        @pl.when(has_left)
        def _():
            landed(h, p)
            acc[...] += arrived[h, p].astype(jnp.float32)

        @pl.when(has_right)
        def _():
            landed(h, C)
            acc[...] += arrived[h, C].astype(jnp.float32)

        for t in range(n):
            out[t * rows + h * r : t * rows + (h + 1) * r, :] = acc[t * r : (t + 1) * r, :].astype(jnp.bfloat16)

    def scatter_drain(h):
        for q in range(C):
            to_peer(h, q).wait_send()
            pl.when(q > p)(lambda: to_right(h, q).wait_send())
            pl.when(q < p)(lambda: to_left(h, q).wait_send())

    def norm(h):
        step = 16

        @pl.loop(0, T // step)
        def _(i):
            at = pl.ds(pl.multiple_of(i * step, step), step)
            wide = every[h, at, :].astype(jnp.float32)
            square_mean = jnp.mean(wide * wide, axis=1, keepdims=True)
            normed[at, :] = (wide * gain[...] / jnp.sqrt(square_mean + 1e-05)).astype(jnp.bfloat16)

    def expand(hooks):
        tile = 256 if F % 256 == 0 else 128

        @pl.loop(0, F // tile)
        def _(i):
            for k, hook in hooks:
                pl.when(i == min(k, F // tile - 1))(hook)
            at = pl.ds(pl.multiple_of(i * tile, tile), tile)
            gate = jnp.dot(normed[...], gwv[:, at], preferred_element_type=jnp.float32)
            up = jnp.dot(normed[...], uwv[:, at], preferred_element_type=jnp.float32)
            hidden[:, at] = (jax.nn.silu(gate) * up).astype(jnp.bfloat16)

    def reduce(h, hooks):
        @pl.loop(0, n)
        def _(i):
            for k, hook in hooks:
                pl.when(i == min(k, n - 1))(hook)
            q = lax.rem(i, C)
            t = 2 * q + jnp.where(i < C, 1 - c, c)
            at = pl.ds(pl.multiple_of(t * width, width), width)
            part[h, t] = jnp.dot(hidden[...], dwv[:, at], preferred_element_type=jnp.float32).astype(jnp.bfloat16)
            pl.when(i < C)(lambda: to_peer(h, q).start())

    gather_first(0)
    for s in range(1, C):
        gather_step(0, s)
    gather_first(1)
    gather_last(0)
    norm(0)
    loads[0].wait()
    loads[1].wait()
    expand([(4, lambda: gather_step(1, 1))])
    loads[2].wait()
    reduce(0, [(2, lambda: gather_step(1, 2)) if C > 2 else (2, lambda: None)])
    scatter_first(0)
    for s in range(3, C):
        gather_step(1, s)
    gather_last(1)
    norm(1)
    expand([(3, lambda: scatter_step(0, 0))])
    reduce(1, [(2, lambda: scatter_step(0, 1))])
    scatter_first(1)
    for j in range(2, C):
        scatter_step(0, j)
    for j in range(C):
        scatter_step(1, j)
    scatter_last(0)
    scatter_last(1)
    for h in range(H):
        gather_drain(h)
        scatter_drain(h)


def on_device(n, tokens, norm_gain, gate_weight, up_weight, down_weight):
    H = HALVES
    rows, D = tokens.shape
    F = gate_weight.shape[1]
    C = n // 2
    T, width = n * rows // H, D // n
    bf16 = jnp.bfloat16
    any_space, vmem = pl.BlockSpec(memory_space=pl.ANY), pl.BlockSpec(memory_space=pltpu.VMEM)
    dma = pltpu.SemaphoreType.DMA
    return pl.pallas_call(
        functools.partial(block_kernel, n),
        out_shape=jax.ShapeDtypeStruct((n * rows, width), bf16),
        in_specs=[any_space, vmem, any_space, any_space, any_space],
        out_specs=vmem,
        scratch_shapes=[
            pltpu.VMEM((D, F), bf16),
            pltpu.VMEM((D, F), bf16),
            pltpu.VMEM((F, D), bf16),
            pltpu.VMEM((H, T, D), bf16),
            pltpu.VMEM((T, D), bf16),
            pltpu.VMEM((T, F), bf16),
            pltpu.VMEM((H, n, T, width), bf16),
            pltpu.VMEM((H, C, T, width), bf16),
            pltpu.VMEM((H, C + 1, T, width), bf16),
            pltpu.VMEM((T, width), jnp.float32),
            dma((3,)),
            dma((H,)),
            dma((H, n)),
            dma((3, H, n)),
            dma((H, C)),
            dma((H, C)),
            dma((H, C)),
            dma((H, C + 1)),
        ],
        compiler_params=pltpu.CompilerParams(collective_id=0, has_side_effects=True, vmem_limit_bytes=VMEM_LIMIT),
    )(tokens, norm_gain[None, :], gate_weight, up_weight, down_weight)


def solution(mesh):
    return jax.shard_map(
        functools.partial(on_device, mesh.shape["tensor"]),
        mesh=mesh,
        in_specs=(
            P(("dp", "tensor"), None),
            P(),
            P(None, "tensor"),
            P(None, "tensor"),
            P("tensor", None),
        ),
        out_specs=P("dp", "tensor"),
        check_vma=False,
    )
```
